32 devices in a mesh: ep: 4 (over y, core), etp: 8 (over z, x).
Axes of the slice: x: 2, y: 2, z: 4, core: 2. Of those that a mesh axis runs over, the one named last changes fastest.
Arguments:
- tokens: bfloat16 [4096, 7168], P(('ep', 'etp')), may hold values from -6 to 6
- expert_ids: int32 [4096, 8], P(('ep', 'etp')), may hold values from 0 to 383, all different within a row; in each aligned block of 128 rows (0 to 127, 128 to 255, ...) at most 3 rows name the same one
- gate_q: int32 [4096, 8], P(('ep', 'etp')), may hold values from 1 to 1024
- w_gate: bfloat16 [4, 7168, 2048], P('ep', None, 'etp'), may hold values from -0.0625 to 0.0625
- w_up: bfloat16 [4, 7168, 2048], P('ep', None, 'etp'), may hold values from -0.0625 to 0.0625
- w_down: bfloat16 [4, 2048, 7168], P('ep', 'etp'), may hold values from -0.125 to 0.125
Outputs:
- mixed: bfloat16 [4096, 7168], P(('ep', 'etp'))
The draws below stay inside these ranges and needn't reach their ends.
Inputs may be any that keep to these rules, and one draw needn't show every extreme that they name: `expert_ids`: each row names 8 different experts; among the 128 rows of one device no expert is named by more than 3 rows.
All inputs are finite; a program needn't handle non-finite values.
Results may differ from the reference program's by a relative error of at most 0.014.
Values may be sent and summed in bfloat16 or wider, within the bound.
A program may use at most 64 MiB of HBM per device.

```python
import math
import jax
import jax.numpy as jnp
import numpy as np
from jax import lax

D = 7168
FF = 2048
EXPERTS_ALL = 384
TOP = 8
TOK_DEV = 128
CAP = 3
EXPERTS_WIN = 4
TOKENS = 4096
N_EP = 4
N_ETP = 8
DEVICES = 32


def plant(entries, stream_key, smallest, largest):
    place = [jax.random.randint(jax.random.fold_in(stream_key, axis), (), 0, length) for axis, length in enumerate(entries.shape)]
    main_axis = entries.shape.index(max(entries.shape))
    next_to = place[:main_axis] + [(place[main_axis] + 1) % entries.shape[main_axis]] + place[main_axis + 1:]
    return entries.at[tuple(place)].set(smallest).at[tuple(next_to)].set(largest)


def block_scale(own_key, extent, split, smallest, largest):
    def one(position, blocks):
        draws = jax.random.uniform(jax.random.fold_in(jax.random.fold_in(own_key, 6), position), (blocks,), jnp.float32, smallest / len(split), largest / len(split))
        return jnp.repeat(jnp.exp(draws), extent[position] // blocks).reshape((-1,) + (1,) * (len(extent) - position - 1))

    loudness = one(*split[0])
    for cut in split[1:]:
        loudness = loudness * one(*cut)
    return loudness


def deal_out(key, own, number, rows, number_of, top, limit, lean):
    sequence = jax.random.permutation(key, number_of)
    heavy_load, ordinary = portions_of(number_of, rows * top, limit, lean, True), portions_of(number_of, rows * top, limit, lean, False)
    places = jnp.arange(number_of)

    def named(sizes, offset_by):
        used = int((sizes > 0).sum())
        fixed = max(1, used // 4)
        shifted = fixed + (places - fixed + offset_by * (used - fixed)) % max(1, number_of - fixed)
        return jnp.zeros((number_of,), jnp.int32).at[sequence[jnp.where(places < fixed, places, shifted)]].set(jnp.asarray(sizes, jnp.int32))

    sizes = jnp.where(number % 4 == 0, named(heavy_load, number // 4), named(ordinary, number - number // 4 - 1))
    mixed = jax.random.permutation(jax.random.fold_in(own, 3), number_of)
    donor, receiver = mixed[0:number_of // 2 * 2:2], mixed[1:number_of // 2 * 2:2]
    room = jnp.minimum(sizes[donor] - 1, limit - sizes[receiver]) // 2
    room = jnp.where((donor == sequence[0]) | (receiver == sequence[0]) | (sizes[receiver] == 0), 0, jnp.maximum(room, 0))
    shifted = jax.random.randint(jax.random.fold_in(own, 4), (number_of // 2,), 0, 1 << 20) % (room + 1)
    sizes = sizes.at[donor].add(-shifted).at[receiver].add(shifted)
    items = jnp.searchsorted(jnp.cumsum(sizes), jnp.arange(rows * top), side="right").astype(jnp.int32)
    listing = items.reshape(top, rows).T
    listing = listing[jax.random.permutation(jax.random.fold_in(own, 1), rows)]
    offset_by = jax.random.randint(jax.random.fold_in(own, 2), (rows, 1), 0, top)
    return jnp.take_along_axis(listing, (jnp.arange(top)[None, :] + offset_by) % top, axis=1)


def portions_of(count, total, reach, lean, full):
    loads = [(1 << 20) // math.isqrt(standing ** lean) + 1 for standing in range(1, count + 1)]
    largest = reach if full else min(reach, max(-(-total // count), total * loads[0] // sum(loads)))
    least = 1 if total - largest >= count - 1 else 0
    holding, surplus = [largest] + [least] * (count - 1), total - largest - least * (count - 1)
    while surplus > 0:
        candidates = [i for i in range(1, count) if holding[i] < largest] or [i for i in range(1, count) if holding[i] < reach]
        mass, left = sum([loads[i] for i in candidates]), surplus
        for i in candidates:
            addition = min(reach - holding[i], max(1, left * loads[i] // mass), surplus)
            holding[i] = holding[i] + addition
            surplus = surplus - addition
    return np.array(holding)


def bell_draw(stream_key, shape, spread, reach, cuts=(), kind=jnp.bfloat16):
    values = jax.random.normal(stream_key, shape, jnp.float32) * spread
    if len(cuts) > 0:
        values = block_scale(stream_key, shape, cuts, -0.22, 0.18) * values
    return jnp.clip(values, min=-reach, max=reach).astype(kind)


def setup_inputs(seed: int = 0) -> dict:
    keys = jax.random.split(jax.random.key(seed), 7)
    tokens = bell_draw(keys[0], (TOKENS, D), 1.0, 6.0, ((0, 32),))
    expert_ids_keys = jax.random.split(jax.random.fold_in(keys[1], 1), TOKENS // TOK_DEV)
    expert_ids_turns = jax.random.permutation(jax.random.fold_in(keys[1], 3), TOKENS // TOK_DEV)
    expert_ids = jax.vmap(lambda own, number: deal_out(jax.random.fold_in(keys[1], 2), own, number, TOK_DEV, EXPERTS_ALL, TOP, CAP, 2))(expert_ids_keys, expert_ids_turns).reshape((TOKENS, TOP))
    gate_q = plant(jax.random.randint(keys[2], (TOKENS, TOP), 1, 1025), jax.random.fold_in(keys[2], 1), 1, 1024).astype(jnp.int32)
    w_gate = bell_draw(keys[3], (EXPERTS_WIN, D, FF), D ** -0.5, 0.0625, ((0, 4), (2, 8)))
    w_up = bell_draw(keys[4], (EXPERTS_WIN, D, FF), D ** -0.5, 0.0625, ((0, 4), (2, 8)))
    w_down = bell_draw(keys[5], (EXPERTS_WIN, FF, D), FF ** -0.5, 0.125, ((0, 4), (1, 8)))
    return dict(tokens=tokens, expert_ids=expert_ids, gate_q=gate_q, w_gate=w_gate, w_up=w_up, w_down=w_down)


def reference(tokens, expert_ids, gate_q, w_gate, w_up, w_down):
    slots = DEVICES * CAP
    group = FF // N_ETP
    weights = gate_q.astype(jnp.float32) / 1024.0

    def one_expert(carry, expert):
        match = expert_ids == expert
        token_weight = jnp.sum(jnp.where(match, weights, jnp.float32(0.0)), axis=1)
        used = jnp.any(match, axis=1)
        index = jnp.nonzero(used, size=slots, fill_value=0)[0].astype(jnp.int32)
        valid = jnp.arange(slots, dtype=jnp.int32) < jnp.sum(used.astype(jnp.int32))
        rows = tokens[index]
        gate = jnp.dot(rows, w_gate[expert], preferred_element_type=jnp.float32)
        upper = jnp.dot(rows, w_up[expert], preferred_element_type=jnp.float32)
        hidden = (jax.nn.silu(gate) * upper).astype(jnp.bfloat16)
        hidden_groups = hidden.reshape(slots, N_ETP, group).transpose(1, 0, 2)
        down_groups = w_down[expert].reshape(N_ETP, group, D)

        def add_group(total, pair):
            part = jnp.dot(pair[0], pair[1], preferred_element_type=jnp.float32).astype(jnp.bfloat16)
            return total + part.astype(jnp.float32), None

        summed, _ = lax.scan(add_group, jnp.zeros((slots, D), jnp.float32), (hidden_groups, down_groups))
        expert_out = summed.astype(jnp.bfloat16).astype(jnp.float32)
        scale = jnp.where(valid, token_weight[index], jnp.float32(0.0))
        carry = carry.at[index].add(scale[:, None] * expert_out)
        return carry, None

    total, _ = lax.scan(one_expert, jnp.zeros((TOKENS, D), jnp.float32), jnp.arange(N_EP, dtype=jnp.int32))
    return total.astype(jnp.bfloat16)
```

```python
import functools

import jax
import jax.numpy as jnp
from jax import lax
from jax.experimental import pallas as pl
from jax.experimental.pallas import tpu as pltpu
from jax.sharding import PartitionSpec as P

CAP = 3
PACK = 4
MESH = pl.DeviceIdType.MESH
F32 = jnp.float32
BF16 = jnp.bfloat16


def split_members(members):
    inner = 1
    while (inner * 2) ** 2 <= members and members % (inner * 2) == 0:
        inner *= 2
    return members // inner, inner


def partner(index, step, count):
    if count & (count - 1):
        return lax.rem(index + step, count)
    out, bit = index, 1
    while bit < count:
        if step & bit:
            out = out + bit - 2 * bit * lax.rem(index // bit, 2)
        bit *= 2
    return out


def slots(ids_ref, columns):
    rows, top = ids_ref.shape
    ids = ids_ref[...]
    column = lax.broadcasted_iota(jnp.int32, (rows, columns), 1)
    expert, lane = column // PACK, column % PACK
    match = jnp.zeros((rows, columns), F32)
    for r in range(top):
        match = match + jnp.where(ids[:, r : r + 1] == expert, 1.0, 0.0)
    first = lax.broadcasted_iota(jnp.int32, (rows, rows), 0)
    second = lax.broadcasted_iota(jnp.int32, (rows, rows), 1)
    lower = jnp.where(second < first, 1.0, 0.0).astype(BF16)
    rank = jnp.dot(lower, match.astype(BF16), preferred_element_type=F32)
    return match, rank, lane, expert


def pick(match, rank, lane, k):
    if k is None:
        return jnp.where((rank == lane.astype(F32)) & (lane < CAP), match, 0.0)
    return jnp.where((rank == k) & (lane == CAP), match, 0.0)


def exchange_kernel(
    sizes, ids_ref, tok_ref, wg_hbm, wu_hbm, wd_hbm, out_ref,
    stage, sendp, recvp, gath, part, xin, zout, zin, backp, backin, wg, wu, wd,
    w_sem, a_send, a_recv, zg_send, zg_recv, xg_send, xg_recv,
    xr_send, xr_recv, zr_send, zr_recv, b_send, b_recv,
):
    EP, Z, X = sizes
    R = PACK * EP
    q = tok_ref.shape[1] // PACK
    me = lax.axis_index("ep")
    m = lax.axis_index("etp")
    z, x = m // X, lax.rem(m, X)

    loads = [
        pltpu.make_async_copy(src, dst, w_sem.at[i])
        for i, (src, dst) in enumerate(((wg_hbm, wg), (wu_hbm, wu), (wd_hbm, wd)))
    ]
    for copy in loads:
        copy.start()

    barrier = pltpu.get_barrier_semaphore()
    eps = [partner(me, s, EP) for s in range(EP)]
    zs = [partner(z, s, Z) for s in range(Z)]
    xs = [partner(x, s, X) for s in range(X)]

    def dev(p=None, zi=None, xi=None):
        zi, xi = z if zi is None else zi, x if xi is None else xi
        return (me if p is None else p, zi * X + xi)

    for s in range(1, EP):
        pl.semaphore_signal(barrier, inc=1, device_id=dev(p=eps[s]), device_id_type=MESH)
    for s in range(1, Z):
        pl.semaphore_signal(barrier, inc=1, device_id=dev(zi=zs[s]), device_id_type=MESH)
    for s in range(1, X):
        pl.semaphore_signal(barrier, inc=1, device_id=dev(xi=xs[s]), device_id_type=MESH)

    columns = -(-R // 128) * 128
    match, rank, lane, _ = slots(ids_ref, columns)
    base = jnp.transpose(pick(match, rank, lane, None))[:R].astype(BF16)
    last = tok_ref[:, CAP * q :]
    for k in range(CAP):
        extra = jnp.transpose(pick(match, rank, lane, k))[:R].astype(BF16)
        cut = pl.ds(k * q, q)
        stage[:, cut] = jnp.dot(base, tok_ref[:, cut], preferred_element_type=F32) + jnp.dot(
            extra, last, preferred_element_type=F32
        )
    for e in range(EP):
        sendp[e] = stage[PACK * e : PACK * (e + 1), :].astype(BF16)

    pl.semaphore_wait(barrier, EP + Z + X - 3)

    pending = []

    def remote(src, dst, ssem, rsem, device):
        copy = pltpu.make_async_remote_copy(
            src_ref=src, dst_ref=dst, send_sem=ssem, recv_sem=rsem,
            device_id=device, device_id_type=MESH,
        )
        copy.start()
        pending.append(copy)

    def arrived(ref, ssem, rsem):
        pltpu.make_async_remote_copy(
            src_ref=ref, dst_ref=ref, send_sem=ssem, recv_sem=rsem,
            device_id=dev(p=eps[-1]), device_id_type=MESH,
        ).wait_recv()

    for s in range(1, EP):
        remote(sendp.at[eps[s]], recvp.at[me], a_send.at[s], a_recv.at[me], dev(p=eps[s]))
    recvp[me] = sendp[me]
    for s in range(1, EP):
        arrived(recvp.at[eps[s]], a_send.at[0], a_recv.at[eps[s]])
    for p in range(EP):
        stage[PACK * p : PACK * (p + 1), :] = recvp[p].astype(F32)
    gath[x, z] = stage[...].astype(BF16)

    def pass_on(zi, s0):
        for s in range(1, X):
            remote(
                gath.at[x, zi], gath.at[x, zi], xg_send.at[s0, s], xg_recv.at[x, zi], dev(xi=xs[s])
            )

    for s in range(1, Z):
        remote(gath.at[x, z], gath.at[x, z], zg_send.at[s], zg_recv.at[z], dev(zi=zs[s]))
    pass_on(z, 0)
    for s in range(1, Z):
        arrived(gath.at[x, zs[s]], zg_send.at[0], zg_recv.at[zs[s]])
        pass_on(zs[s], s)
    for copy in loads[:2]:
        copy.wait()
    for s in range(1, X):
        for t in range(Z):
            arrived(gath.at[xs[s], zs[t]], xg_send.at[0, 0], xg_recv.at[xs[s], zs[t]])
    loads[2].wait()

    rows = Z * R
    inner = wg.shape[1]
    hidden = []
    group = X if X * rows <= 128 else 1
    row = lax.broadcasted_iota(jnp.int32, (group * rows, 1), 0) % PACK

    def unpack_dot(a, w):
        total = None
        for k in range(CAP):
            piece = a[:, k * q : (k + 1) * q]
            main = jnp.dot(piece, w[k * q : (k + 1) * q, :], preferred_element_type=F32)
            total = main if total is None else total + main
            tail = jnp.dot(piece, w[CAP * q :, :], preferred_element_type=F32)
            tail = pltpu.roll(tail, group * rows - (CAP - k), 0)
            total = total + jnp.where(row == k, tail, 0.0)
        return total

    def work(g, carry):
        a = gath[pl.ds(g * group, group)].reshape(group * rows, CAP * q)
        gate = unpack_dot(a, wg)
        upper = unpack_dot(a, wu)
        hid = (gate / (1.0 + jnp.exp(-gate)) * upper).astype(BF16)
        for k in range(CAP):
            main = jnp.dot(hid, wd[:, k * q : (k + 1) * q], preferred_element_type=F32)
            tail = jnp.dot(hid, wd[:, CAP * q :], preferred_element_type=F32)
            tail = pltpu.roll(tail, CAP - k, 0)
            both = jnp.where(row == CAP, tail, main)
            part[pl.ds(g * group, group), :, :, k * q : (k + 1) * q] = both.astype(BF16).reshape(
                group, Z, R, q
            )
            if group == X:
                send_x(k)
        return carry

    order = list(range(Z - 1, -1, -1))

    def send_x(k):
        cut = pl.ds(k * q, q)
        for t in order:
            for s in range(1, X):
                remote(
                    part.at[xs[s], zs[t], :, cut], xin.at[x, zs[t], :, cut],
                    xr_send.at[s, t, k], xr_recv.at[x, zs[t], k], dev(xi=xs[s]),
                )

    if group == X:
        work(0, 0)
    else:
        lax.fori_loop(0, X, work, 0)
        for k in range(CAP):
            send_x(k)

    for k in range(CAP):
        cut = pl.ds(k * q, q)
        for t in order:
            total = part[x, zs[t], :, cut].astype(F32)
            for s in range(1, X):
                arrived(
                    xin.at[xs[s], zs[t], :, cut], xr_send.at[0, 0, 0], xr_recv.at[xs[s], zs[t], k]
                )
                total = total + xin[xs[s], zs[t], :, cut].astype(F32)
            if t:
                zout[zs[t], :, cut] = total.astype(BF16)
                remote(
                    zout.at[zs[t], :, cut], zin.at[z, :, cut],
                    zr_send.at[t, k], zr_recv.at[z, k], dev(zi=zs[t]),
                )
            else:
                stage[:, cut] = total
    for k in range(CAP):
        cut = pl.ds(k * q, q)
        total = stage[:, cut]
        for t in range(1, Z):
            arrived(zin.at[zs[t], :, cut], zr_send.at[0, 0], zr_recv.at[zs[t], k])
            total = total + zin[zs[t], :, cut].astype(F32)
        stage[:, cut] = total
        for p in range(EP):
            backp[p, :, cut] = stage[PACK * p : PACK * (p + 1), cut].astype(BF16)
        for s in range(1, EP):
            remote(
                backp.at[eps[s], :, cut], backin.at[me, :, cut],
                b_send.at[s, k], b_recv.at[me, k], dev(p=eps[s]),
            )
        backin[me, :, cut] = backp[me, :, cut]
    for k in range(CAP):
        cut = pl.ds(k * q, q)
        for s in range(1, EP):
            arrived(backin.at[eps[s], :, cut], b_send.at[0, 0], b_recv.at[eps[s], k])
        for p in range(EP):
            stage[PACK * p : PACK * (p + 1), cut] = backin[p, :, cut].astype(F32)
        out_ref[:, cut] = stage[:, cut].astype(BF16)
    for copy in pending:
        copy.wait_send()


def mix_kernel(ids_ref, gate_ref, rows_ref, out_ref):
    R = rows_ref.shape[0]
    q = rows_ref.shape[1] // CAP
    top = ids_ref.shape[1]
    match, rank, lane, expert = slots(ids_ref, R)
    ids, units = ids_ref[...], gate_ref[...]
    coarse = (units // 32) * 32
    hi = jnp.zeros(match.shape, F32)
    lo = jnp.zeros(match.shape, F32)
    for r in range(top):
        here = ids[:, r : r + 1] == expert
        hi = hi + jnp.where(here, coarse[:, r : r + 1].astype(F32), 0.0)
        lo = lo + jnp.where(here, (units - coarse)[:, r : r + 1].astype(F32), 0.0)
    hi, lo = hi / 1024.0, lo / 1024.0

    def weighted(mask, piece):
        return jnp.dot((hi * mask).astype(BF16), piece, preferred_element_type=F32) + jnp.dot(
            (lo * mask).astype(BF16), piece, preferred_element_type=F32
        )

    tail = None
    for k in range(CAP):
        piece = rows_ref[:, k * q : (k + 1) * q]
        out_ref[:, k * q : (k + 1) * q] = weighted(pick(match, rank, lane, None), piece).astype(BF16)
        term = weighted(pick(match, rank, lane, k), piece)
        tail = term if tail is None else tail + term
    out_ref[:, CAP * q :] = tail.astype(BF16)


def body(sizes, tokens, expert_ids, gate_q, w_gate, w_up, w_down):
    EP, Z, X = sizes
    R = PACK * EP
    count, width = tokens.shape
    q = width // PACK
    W = CAP * q
    inner = w_gate.shape[2]
    vmem = pl.BlockSpec(memory_space=pltpu.VMEM)
    hbm = pl.BlockSpec(memory_space=pl.ANY)
    dma = pltpu.SemaphoreType.DMA
    rows = pl.pallas_call(
        functools.partial(exchange_kernel, sizes),
        out_shape=jax.ShapeDtypeStruct((R, W), BF16),
        in_specs=[vmem, vmem, hbm, hbm, hbm],
        out_specs=vmem,
        scratch_shapes=[
            pltpu.VMEM((R, W), F32),
            pltpu.VMEM((EP, PACK, W), BF16),
            pltpu.VMEM((EP, PACK, W), BF16),
            pltpu.VMEM((X, Z, R, W), BF16),
            pltpu.VMEM((X, Z, R, W), BF16),
            pltpu.VMEM((X, Z, R, W), BF16),
            pltpu.VMEM((Z, R, W), BF16),
            pltpu.VMEM((Z, R, W), BF16),
            pltpu.VMEM((EP, PACK, W), BF16),
            pltpu.VMEM((EP, PACK, W), BF16),
            pltpu.VMEM((width, inner), BF16),
            pltpu.VMEM((width, inner), BF16),
            pltpu.VMEM((inner, width), BF16),
            dma((3,)),
            dma((EP,)), dma((EP,)),
            dma((Z,)), dma((Z,)),
            dma((Z, X)), dma((X, Z)),
            dma((X, Z, CAP)), dma((X, Z, CAP)),
            dma((Z, CAP)), dma((Z, CAP)),
            dma((EP, CAP)), dma((EP, CAP)),
        ],
        compiler_params=pltpu.CompilerParams(
            collective_id=0, has_side_effects=True, vmem_limit_bytes=64_000_000
        ),
    )(expert_ids, tokens, w_gate[0], w_up[0], w_down[0])
    return pl.pallas_call(
        mix_kernel,
        out_shape=jax.ShapeDtypeStruct((count, width), BF16),
        in_specs=[vmem, vmem, vmem],
        out_specs=vmem,
    )(expert_ids, gate_q, rows)


def solution(mesh):
    in_specs = (
        P(("ep", "etp"), None),
        P(("ep", "etp"), None),
        P(("ep", "etp"), None),
        P("ep", None, "etp"),
        P("ep", None, "etp"),
        P("ep", "etp", None),
    )
    sizes = (mesh.shape["ep"],) + split_members(mesh.shape["etp"])
    out_specs = P(("ep", "etp"), None)
    return jax.shard_map(
        functools.partial(body, sizes), mesh=mesh, in_specs=in_specs, out_specs=out_specs,
        check_vma=False,
    )
```

```python
import functools

import jax
import jax.numpy as jnp
from jax import lax
from jax.experimental import pallas as pl
from jax.experimental.pallas import tpu as pltpu
from jax.sharding import PartitionSpec as P

CAP = 3
PACK = 4
MESH = pl.DeviceIdType.MESH
F32 = jnp.float32
BF16 = jnp.bfloat16


def split_members(members):
    inner = 1
    while (inner * 2) ** 2 <= members and members % (inner * 2) == 0:
        inner *= 2
    return members // inner, inner


def partner(index, step, count):
    if count & (count - 1):
        return lax.rem(index + step, count)
    out, bit = index, 1
    while bit < count:
        if step & bit:
            out = out + bit - 2 * bit * lax.rem(index // bit, 2)
        bit *= 2
    return out


def slots(ids_ref, columns):
    top, rows = ids_ref.shape
    ids = ids_ref[...]
    column = lax.broadcasted_iota(jnp.int32, (columns, rows), 0)
    expert, lane = column // PACK, column % PACK
    match = jnp.zeros((columns, rows), F32)
    for r in range(top):
        match = match + jnp.where(ids[r : r + 1, :] == expert, 1.0, 0.0)
    first = lax.broadcasted_iota(jnp.int32, (rows, rows), 0)
    second = lax.broadcasted_iota(jnp.int32, (rows, rows), 1)
    upper = jnp.where(first < second, 1.0, 0.0).astype(BF16)
    rank = jnp.dot(match.astype(BF16), upper, preferred_element_type=F32)
    return match, rank, lane, expert


def pick(match, rank, lane, k):
    if k is None:
        return jnp.where((rank == lane.astype(F32)) & (lane < CAP), match, 0.0)
    return jnp.where((rank == k) & (lane == CAP), match, 0.0)


def exchange_kernel(
    sizes, ids_ref, gate_ref, tok_hbm, wg_hbm, wu_hbm, wd_hbm, out_ref, mix_ref,
    tok_ref, stage, sendp, recvp, gath, part, xin, zout, zin, backp, backin, wg, wu, wd,
    w_sem, t_sem, a_send, a_recv, zg_send, zg_recv, xg_send, xg_recv,
    xr_send, xr_recv, zr_send, zr_recv, b_send, b_recv,
):
    EP, Z, X = sizes
    R = PACK * EP
    q = tok_ref.shape[1] // PACK
    me = lax.axis_index("ep")
    m = lax.axis_index("etp")
    z, x = m // X, lax.rem(m, X)
    eps = [partner(me, s, EP) for s in range(EP)]
    zs = [partner(z, s, Z) for s in range(Z)]
    xs = [partner(x, s, X) for s in range(X)]
    cuts = [pl.ds(k * q, q) for k in range(PACK)]

    def dev(p=None, zi=None, xi=None):
        zi, xi = z if zi is None else zi, x if xi is None else xi
        return (me if p is None else p, zi * X + xi)

    barrier = pltpu.get_barrier_semaphore()
    for s in range(1, EP):
        pl.semaphore_signal(barrier, inc=1, device_id=dev(p=eps[s]), device_id_type=MESH)
    for s in range(1, Z):
        pl.semaphore_signal(barrier, inc=1, device_id=dev(zi=zs[s]), device_id_type=MESH)
    for s in range(1, X):
        pl.semaphore_signal(barrier, inc=1, device_id=dev(xi=xs[s]), device_id_type=MESH)

    feeds = [
        pltpu.make_async_copy(tok_hbm.at[:, cuts[k]], tok_ref.at[:, cuts[k]], t_sem.at[k])
        for k in range(PACK)
    ]
    loads = [
        pltpu.make_async_copy(src, dst, w_sem.at[i])
        for i, (src, dst) in enumerate(((wg_hbm, wg), (wu_hbm, wu), (wd_hbm, wd)))
    ]
    for copy in feeds[::-1] + loads:
        copy.start()

    pending = []

    def remote(src, dst, ssem, rsem, device):
        copy = pltpu.make_async_remote_copy(
            src_ref=src, dst_ref=dst, send_sem=ssem, recv_sem=rsem,
            device_id=device, device_id_type=MESH,
        )
        copy.start()
        pending.append(copy)

    def arrived(ref, ssem, rsem):
        pltpu.make_async_remote_copy(
            src_ref=ref, dst_ref=ref, send_sem=ssem, recv_sem=rsem,
            device_id=dev(p=eps[-1]), device_id_type=MESH,
        ).wait_recv()

    match, rank, lane, expert = slots(ids_ref, R)
    base = pick(match, rank, lane, None)
    extras = [pick(match, rank, lane, k) for k in range(CAP)]
    feeds[CAP].wait()
    for k in range(CAP - 1, -1, -1):
        cut = cuts[k]
        feeds[k].wait()
        stage[:, cut] = jnp.dot(
            base.astype(BF16), tok_ref[:, cut], preferred_element_type=F32
        ) + jnp.dot(extras[k].astype(BF16), tok_ref[:, cuts[CAP]], preferred_element_type=F32)
        for e in range(EP):
            sendp[e, :, cut] = stage[PACK * e : PACK * (e + 1), cut].astype(BF16)
        if k == CAP - 1:
            pl.semaphore_wait(barrier, EP + Z + X - 3)
        for s in range(1, EP):
            remote(
                sendp.at[eps[s], :, cut], recvp.at[me, :, cut],
                a_send.at[s, k], a_recv.at[me, k], dev(p=eps[s]),
            )
        recvp[me, :, cut] = sendp[me, :, cut]

    def pass_on(zi, s0, k):
        for s in range(1, X):
            remote(
                gath.at[x, zi, :, cuts[k]], gath.at[x, zi, :, cuts[k]],
                xg_send.at[s0, s, k], xg_recv.at[x, zi, k], dev(xi=xs[s]),
            )

    for k in range(CAP - 1, -1, -1):
        cut = cuts[k]
        for s in range(1, EP):
            arrived(recvp.at[eps[s], :, cut], a_send.at[0, 0], a_recv.at[eps[s], k])
        for p in range(EP):
            stage[PACK * p : PACK * (p + 1), cut] = recvp[p, :, cut].astype(F32)
        gath[x, z, :, cut] = stage[:, cut].astype(BF16)
        for s in range(1, Z):
            remote(
                gath.at[x, z, :, cut], gath.at[x, z, :, cut],
                zg_send.at[s, k], zg_recv.at[z, k], dev(zi=zs[s]),
            )
        pass_on(z, 0, k)

    units = gate_ref[...]
    coarse = (units // 32) * 32
    hi = jnp.zeros(match.shape, F32)
    lo = jnp.zeros(match.shape, F32)
    for r in range(ids_ref.shape[0]):
        here = ids_ref[r : r + 1, :] == expert
        hi = hi + jnp.where(here, coarse[r : r + 1, :].astype(F32), 0.0)
        lo = lo + jnp.where(here, (units - coarse)[r : r + 1, :].astype(F32), 0.0)
    hi, lo = hi / 1024.0, lo / 1024.0
    parts = [w * mask for mask in [base] + extras for w in (hi, lo)]
    mix_ref[...] = jnp.transpose(jnp.concatenate(parts, axis=0)).astype(BF16)

    def relay(k):
        for s in range(1, Z):
            arrived(gath.at[x, zs[s], :, cuts[k]], zg_send.at[0, 0], zg_recv.at[zs[s], k])
            pass_on(zs[s], s, k)

    def gathered(k):
        for t in range(Z):
            for s in range(1, X):
                arrived(
                    gath.at[xs[s], zs[t], :, cuts[k]], xg_send.at[0, 0, 0],
                    xg_recv.at[xs[s], zs[t], k],
                )

    group = X if X * Z * R <= 128 else 1
    count = group * Z * R
    row = lax.broadcasted_iota(jnp.int32, (count, 1), 0) % PACK

    def enter(g, k, w, total):
        a = gath[pl.ds(g * group, group), :, :, cuts[k]].reshape(count, q)
        main = jnp.dot(a, w[k * q : (k + 1) * q, :], preferred_element_type=F32)
        tail = jnp.dot(a, w[CAP * q :, :], preferred_element_type=F32)
        tail = pltpu.roll(tail, count - (CAP - k), 0)
        main = main + jnp.where(row == k, tail, 0.0)
        return main if total is None else total + main

    def leave(g, gate, upper):
        hid = (gate / (1.0 + jnp.exp(-gate)) * upper).astype(BF16)
        last = jnp.dot(hid, wd[:, cuts[CAP]], preferred_element_type=F32)
        for k in range(CAP):
            main = jnp.dot(hid, wd[:, cuts[k]], preferred_element_type=F32)
            both = jnp.where(row == CAP, pltpu.roll(last, CAP - k, 0), main)
            part[pl.ds(g * group, group), :, :, cuts[k]] = both.astype(BF16).reshape(
                group, Z, R, q
            )
            if group == X:
                send_x(k)

    order = list(range(Z - 1, -1, -1))

    def send_x(k):
        cut = pl.ds(k * q, q)
        for t in order:
            for s in range(1, X):
                remote(
                    part.at[xs[s], zs[t], :, cut], xin.at[x, zs[t], :, cut],
                    xr_send.at[s, t, k], xr_recv.at[x, zs[t], k], dev(xi=xs[s]),
                )

    def ready():
        for copy in loads:
            copy.wait()

    if group == X:
        gate = upper = None
        for step in range(CAP + 1):
            if step < CAP:
                relay(CAP - 1 - step)
            if step == 1:
                ready()
            if step:
                k = CAP - step
                gathered(k)
                gate = enter(0, k, wg, gate)
                upper = enter(0, k, wu, upper)
        leave(0, gate, upper)
    else:
        for k in range(CAP):
            relay(k)
        for k in range(CAP):
            gathered(k)
        ready()

        def work(g, carry):
            gate = upper = None
            for k in range(CAP):
                gate = enter(g, k, wg, gate)
                upper = enter(g, k, wu, upper)
            leave(g, gate, upper)
            return carry

        lax.fori_loop(0, X, work, 0)
        for k in range(CAP):
            send_x(k)

    for k in range(CAP):
        cut = pl.ds(k * q, q)
        for t in order:
            total = part[x, zs[t], :, cut].astype(F32)
            for s in range(1, X):
                arrived(
                    xin.at[xs[s], zs[t], :, cut], xr_send.at[0, 0, 0], xr_recv.at[xs[s], zs[t], k]
                )
                total = total + xin[xs[s], zs[t], :, cut].astype(F32)
            if t:
                zout[zs[t], :, cut] = total.astype(BF16)
                remote(
                    zout.at[zs[t], :, cut], zin.at[z, :, cut],
                    zr_send.at[t, k], zr_recv.at[z, k], dev(zi=zs[t]),
                )
            else:
                stage[:, cut] = total
    for k in range(CAP):
        cut = pl.ds(k * q, q)
        total = stage[:, cut]
        for t in range(1, Z):
            arrived(zin.at[zs[t], :, cut], zr_send.at[0, 0], zr_recv.at[zs[t], k])
            total = total + zin[zs[t], :, cut].astype(F32)
        stage[:, cut] = total
        for p in range(EP):
            backp[p, :, cut] = stage[PACK * p : PACK * (p + 1), cut].astype(BF16)
        for s in range(1, EP):
            remote(
                backp.at[eps[s], :, cut], backin.at[me, :, cut],
                b_send.at[s, k], b_recv.at[me, k], dev(p=eps[s]),
            )
        backin[me, :, cut] = backp[me, :, cut]
    for k in range(CAP):
        cut = pl.ds(k * q, q)
        for s in range(1, EP):
            arrived(backin.at[eps[s], :, cut], b_send.at[0, 0], b_recv.at[eps[s], k])
        for p in range(EP):
            stage[PACK * p : PACK * (p + 1), cut] = backin[p, :, cut].astype(F32)
        out_ref[:R, cut] = stage[:, cut].astype(BF16)
        out_ref[R:, cut] = stage[:, cut].astype(BF16)
    for copy in pending:
        copy.wait_send()


def mix_kernel(mix_ref, rows_ref, out_hbm, out, sem):
    R2 = rows_ref.shape[0]
    q = rows_ref.shape[1] // CAP
    copies = []
    tail = None

    def emit(k, value):
        cut = pl.ds(k * q, q)
        out[:, cut] = value.astype(BF16)
        copies.append(pltpu.make_async_copy(out.at[:, cut], out_hbm.at[:, cut], sem.at[k]))
        copies[-1].start()

    for k in range(CAP):
        piece = rows_ref[:, k * q : (k + 1) * q]
        emit(k, jnp.dot(mix_ref[:, :R2], piece, preferred_element_type=F32))
        weights = mix_ref[:, (k + 1) * R2 : (k + 2) * R2]
        term = jnp.dot(weights, piece, preferred_element_type=F32)
        tail = term if tail is None else tail + term
    emit(CAP, tail)
    for copy in copies:
        copy.wait()


def body(sizes, tokens, expert_ids, gate_q, w_gate, w_up, w_down):
    EP, Z, X = sizes
    R = PACK * EP
    count, width = tokens.shape
    q = width // PACK
    W = CAP * q
    inner = w_gate.shape[2]
    vmem = pl.BlockSpec(memory_space=pltpu.VMEM)
    hbm = pl.BlockSpec(memory_space=pl.ANY)
    dma = pltpu.SemaphoreType.DMA
    rows, mix = pl.pallas_call(
        functools.partial(exchange_kernel, sizes),
        out_shape=(
            jax.ShapeDtypeStruct((2 * R, W), BF16),
            jax.ShapeDtypeStruct((count, 2 * PACK * R), BF16),
        ),
        in_specs=[vmem, vmem, hbm, hbm, hbm, hbm],
        out_specs=(vmem, vmem),
        scratch_shapes=[
            pltpu.VMEM((count, width), BF16),
            pltpu.VMEM((R, W), F32),
            pltpu.VMEM((EP, PACK, W), BF16),
            pltpu.VMEM((EP, PACK, W), BF16),
            pltpu.VMEM((X, Z, R, W), BF16),
            pltpu.VMEM((X, Z, R, W), BF16),
            pltpu.VMEM((X, Z, R, W), BF16),
            pltpu.VMEM((Z, R, W), BF16),
            pltpu.VMEM((Z, R, W), BF16),
            pltpu.VMEM((EP, PACK, W), BF16),
            pltpu.VMEM((EP, PACK, W), BF16),
            pltpu.VMEM((width, inner), BF16),
            pltpu.VMEM((width, inner), BF16),
            pltpu.VMEM((inner, width), BF16),
            dma((3,)),
            dma((PACK,)),
            dma((EP, CAP)), dma((EP, CAP)),
            dma((Z, CAP)), dma((Z, CAP)),
            dma((Z, X, CAP)), dma((X, Z, CAP)),
            dma((X, Z, CAP)), dma((X, Z, CAP)),
            dma((Z, CAP)), dma((Z, CAP)),
            dma((EP, CAP)), dma((EP, CAP)),
        ],
        compiler_params=pltpu.CompilerParams(
            collective_id=0, has_side_effects=True, vmem_limit_bytes=64_000_000
        ),
    )(expert_ids.T, gate_q.T, tokens, w_gate[0], w_up[0], w_down[0])
    return pl.pallas_call(
        mix_kernel,
        out_shape=jax.ShapeDtypeStruct((count, width), BF16),
        in_specs=[vmem, vmem],
        out_specs=hbm,
        scratch_shapes=[pltpu.VMEM((count, width), BF16), dma((PACK,))],
    )(mix, rows)


def solution(mesh):
    in_specs = (
        P(("ep", "etp"), None),
        P(("ep", "etp"), None),
        P(("ep", "etp"), None),
        P("ep", None, "etp"),
        P("ep", None, "etp"),
        P("ep", "etp", None),
    )
    sizes = (mesh.shape["ep"],) + split_members(mesh.shape["etp"])
    out_specs = P(("ep", "etp"), None)
    return jax.shard_map(
        functools.partial(body, sizes), mesh=mesh, in_specs=in_specs, out_specs=out_specs,
        check_vma=False,
    )
```
